32 devices in a mesh: row: 4 (over z), col: 8 (over y, x, core).
Axes of the slice: x: 2, y: 2, z: 4, core: 2. Of those that a mesh axis runs over, the one named last changes fastest.
Arguments:
- pencil_a: float32 [4, 3072, 8, 1536], P('row', None, 'col'), may hold values from -6 to 6, as said below
- pencil_b: float32 [4, 3072, 8, 1536], P('row', None, 'col'), may hold values from -6 to 6
Outputs:
- new_a: float32 [4, 3072, 8, 1536], P('row', None, 'col')
- new_b: float32 [4, 3072, 8, 1536], P('row', None, 'col')
The draws below stay inside these ranges and needn't reach their ends.
Inputs may be any that keep to these rules, and one draw needn't show every extreme that they name: `pencil_a`: the first 256 columns of Amat are zero in the last 256 rows of Amat.
All inputs are finite; a program needn't handle non-finite values.
Results may differ from the reference program's by a relative error of at most 0.000056.
Values sent between devices are 32-bit elements; how exact they have to be, the bound alone decides.
A program may use at most 192 MiB of HBM per device.

```python
import math
import jax
import jax.numpy as jnp
from jax import lax

N = 12288
NB = 256
N_ROW = 4
N_COL = 8


decay_ratio = 3.0


def to_storage(matrix):
    six = matrix.reshape(N // (NB * N_ROW), N_ROW, NB, N // (NB * N_COL), N_COL, NB)
    return six.transpose(1, 0, 2, 4, 3, 5).reshape(N_ROW, N // N_ROW, N_COL, N // N_COL)


def base_field(key):
    return jax.random.normal(key, (N, N), jnp.float32)


def decay_scales():
    fraction = jnp.arange(NB, dtype=jnp.float32) / (NB - 1)
    return jnp.exp(-math.log(decay_ratio) * fraction)


def reflect_columns(block, key):
    direction = jax.random.normal(key, (NB,), jnp.float32)
    direction = direction / jnp.sqrt(jnp.sum(direction * direction))
    along = jnp.dot(block, direction, precision=lax.Precision.HIGHEST)
    return block - 2.0 * jnp.outer(along, direction)


def draw_pencil_a(key, part):
    inner_key = jax.random.fold_in(key, 11)
    field_key, first_key, second_key = jax.random.split(inner_key, 3)
    matrix = base_field(field_key)
    panel = matrix[:, :NB] * decay_scales()[None, :]
    panel = reflect_columns(panel, first_key)
    panel = reflect_columns(panel, second_key)
    kept_rows = (jnp.arange(N) < N - NB).astype(jnp.float32)[:, None]
    matrix = matrix.at[:, :NB].set(panel * kept_rows)
    return to_storage(jnp.clip(matrix, -6.0, 6.0))


def draw_pencil_b(key, part):
    inner_key = jax.random.fold_in(key, 23)
    field_key, first_key, second_key = jax.random.split(inner_key, 3)
    matrix = base_field(field_key)
    strip_rows = matrix[N - NB:, :] * decay_scales()[:, None]
    mixed_t = reflect_columns(strip_rows.T, first_key)
    mixed_t = reflect_columns(mixed_t, second_key)
    matrix = matrix.at[N - NB:, :].set(mixed_t.T)
    return to_storage(jnp.clip(matrix, -6.0, 6.0))


def setup_inputs(seed: int = 0) -> dict:
    key_list = jax.random.split(jax.random.key(seed), 3)
    pencil_a = draw_pencil_a(jax.random.fold_in(key_list[2], 71), 0)
    pencil_b = draw_pencil_b(jax.random.fold_in(key_list[2], 71), 0)
    return dict(pencil_a=pencil_a, pencil_b=pencil_b)


def matmul(left, right):
    return jnp.dot(left.astype(jnp.float32), right.astype(jnp.float32), precision=lax.Precision.HIGHEST, preferred_element_type=jnp.float32)

def inverse_factor(gram):
    lower = jnp.linalg.cholesky(gram)
    ident = jnp.eye(gram.shape[0], dtype=jnp.float32)
    return jax.scipy.linalg.solve_triangular(lower, ident, lower=True).T

def general_inverse(square):
    lower = jnp.linalg.cholesky(matmul(square, square.T))
    ident = jnp.eye(square.shape[0], dtype=jnp.float32)
    linv = jax.scipy.linalg.solve_triangular(lower, ident, lower=True)
    return matmul(square.T, matmul(linv.T, linv))

def to_matrix(stored):
    six = stored.reshape(N_ROW, N // (NB * N_ROW), NB, N_COL, N // (NB * N_COL), NB)
    return six.transpose(1, 0, 2, 4, 3, 5).reshape(N, N)

def to_stored(matrix):
    six = matrix.reshape(N // (NB * N_ROW), N_ROW, NB, N // (NB * N_COL), N_COL, NB)
    return six.transpose(1, 0, 2, 4, 3, 5).reshape(N_ROW, N // N_ROW, N_COL, N // N_COL)

def reference(pencil_a, pencil_b):
    amat = to_matrix(pencil_a)
    bmat = to_matrix(pencil_b)
    ident = jnp.eye(NB, dtype=jnp.float32)
    panel = amat[:, :NB]
    first_inv = inverse_factor(matmul(panel.T, panel))
    basis = matmul(panel, first_inv)
    kinv_left = general_inverse(ident + basis[:NB])
    vectors = basis.at[:NB].add(ident)
    amat = amat - matmul(vectors, matmul(kinv_left, matmul(vectors.T, amat)))
    bmat = bmat - matmul(vectors, matmul(kinv_left, matmul(vectors.T, bmat)))
    strip = bmat[N - NB:]
    first_inv = inverse_factor(matmul(strip, strip.T))
    basis_t = matmul(first_inv.T, strip)
    kinv_right = general_inverse(ident + basis_t[:, N - NB:].T)
    vectors_t = basis_t.at[:, N - NB:].add(ident)
    amat = amat - matmul(matmul(matmul(amat, vectors_t.T), kinv_right.T), vectors_t)
    bmat = bmat - matmul(matmul(matmul(bmat, vectors_t.T), kinv_right.T), vectors_t)
    return (to_stored(amat), to_stored(bmat))
```

```python
import functools
import jax
import jax.numpy as jnp
from jax import lax
from jax.experimental import pallas as pl
from jax.experimental.pallas import tpu as pltpu
from jax.sharding import PartitionSpec as P

NB = 256
LANES = 128
SUB = 8
F32 = jnp.float32
BF16 = jnp.bfloat16
MIB = 1 << 20


def matmul(left, right):
    return jnp.dot(left, right, precision=lax.Precision.HIGHEST, preferred_element_type=F32)


def split(x):
    hi = x.astype(BF16)
    return hi, (x - hi.astype(F32)).astype(BF16)


def split_out(x):
    hi = lax.reduce_precision(x, 8, 7)
    return hi.astype(BF16), (x - hi).astype(BF16)


def dot_t(left, right, dims):
    return lax.dot_general(left, right, (dims, ((), ())), preferred_element_type=F32)


def dot3(left, right, dims=((1,), (0,))):
    lh, ll = left
    rh, rl = right
    return dot_t(lh, rh, dims) + (dot_t(lh, rl, dims) + dot_t(ll, rh, dims))


def load_cols(ref, first, count, rows, per_row):
    parts = [ref[pl.ds(first + k, rows, stride=per_row), :] for k in range(count)]
    return jnp.concatenate(parts, axis=1)


def left_products_kernel(rows_blk, per_row, pt_ref, raw_ref, out_ref):
    step = pl.program_id(0)

    @pl.when(step == 0)
    def _():
        out_ref[...] = jnp.zeros_like(out_ref)

    pt = split(pt_ref[...])
    group = 2
    for first in range(0, per_row, group):
        block = split(load_cols(raw_ref, first, group, rows_blk, per_row))
        cols = pl.ds(first * LANES, group * LANES)
        out_ref[:, cols] += dot3(pt, block)


def left_products(panel_t, raw, rows, cols, rows_blk):
    width = panel_t.shape[0]
    per_row = cols // LANES
    return pl.pallas_call(
        functools.partial(left_products_kernel, rows_blk, per_row),
        grid=(rows // rows_blk,),
        out_shape=jax.ShapeDtypeStruct((width, cols), F32),
        in_specs=[
            pl.BlockSpec((width, rows_blk), lambda i: (0, i)),
            pl.BlockSpec((rows_blk * per_row, LANES), lambda i: (i, 0)),
        ],
        out_specs=pl.BlockSpec((width, cols), lambda i: (0, 0)),
        compiler_params=pltpu.CompilerParams(vmem_limit_bytes=48 * MIB),
        cost_estimate=pl.CostEstimate(
            flops=6 * width * rows * cols, bytes_accessed=4 * rows * cols, transcendentals=0
        ),
        name="left_products",
    )(panel_t, raw)


def right_products_kernel(rows_blk, per_row, whi_ref, wlo_ref, a_ref, b_ref, out_ref):
    width = whi_ref.shape[1]
    group = 2
    for side, raw_ref in enumerate((a_ref, b_ref)):
        total = None
        for first in range(0, per_row, group):
            block = split(load_cols(raw_ref, first, group, rows_blk, per_row))
            rows = pl.ds(first * LANES, group * LANES)
            term = dot3(block, (whi_ref[rows, :], wlo_ref[rows, :]))
            total = term if total is None else total + term
        out_ref[:, side * width : (side + 1) * width] = total


def right_products(wt, raw_a, raw_b, rows, cols, rows_blk):
    width = wt.shape[1]
    per_row = cols // LANES
    raw_spec = pl.BlockSpec((rows_blk * per_row, LANES), lambda i: (i, 0))
    wide = pl.BlockSpec((cols, width), lambda i: (0, 0))
    whi, wlo = split_out(wt)
    return pl.pallas_call(
        functools.partial(right_products_kernel, rows_blk, per_row),
        grid=(rows // rows_blk,),
        out_shape=jax.ShapeDtypeStruct((rows, 2 * width), F32),
        in_specs=[wide, wide, raw_spec, raw_spec],
        out_specs=pl.BlockSpec((rows_blk, 2 * width), lambda i: (i, 0)),
        compiler_params=pltpu.CompilerParams(vmem_limit_bytes=48 * MIB),
        cost_estimate=pl.CostEstimate(
            flops=12 * width * rows * cols, bytes_accessed=8 * rows * cols, transcendentals=0
        ),
        name="right_products",
    )(whi, wlo, raw_a, raw_b)


def update_kernel(rows_blk, per_row, v_ref, s_ref, dhi_ref, dlo_ref, raw_ref, out_ref):
    width = v_ref.shape[1]
    left = (split(v_ref[...]), split(s_ref[...]))
    group = 2
    for first in range(0, per_row, group):
        cols = pl.ds(first * LANES, group * LANES)
        total = None
        for part in range(2):
            rows = pl.ds(part * width, width)
            term = dot3(left[part], (dhi_ref[rows, cols], dlo_ref[rows, cols]))
            total = term if total is None else total + term
        for k in range(group):
            where = pl.ds(first + k, rows_blk, stride=per_row)
            out_ref[where, :] = raw_ref[where, :] - total[:, k * LANES : (k + 1) * LANES]


def update(vectors, mixed, side, low, raw, rows, cols, rows_blk):
    width = vectors.shape[1]
    per_row = cols // LANES
    raw_spec = pl.BlockSpec((rows_blk * per_row, LANES), lambda i: (i, 0))
    low_spec = pl.BlockSpec((2 * width, cols), lambda i: (0, 0))
    dhi, dlo = split_out(low)
    return pl.pallas_call(
        functools.partial(update_kernel, rows_blk, per_row),
        grid=(rows // rows_blk,),
        out_shape=jax.ShapeDtypeStruct((rows * per_row, LANES), F32),
        in_specs=[
            pl.BlockSpec((rows_blk, width), lambda i: (i, 0)),
            pl.BlockSpec((rows_blk, width), lambda i, side=side: (i, side)),
            low_spec,
            low_spec,
            raw_spec,
        ],
        out_specs=raw_spec,
        compiler_params=pltpu.CompilerParams(vmem_limit_bytes=48 * MIB),
        cost_estimate=pl.CostEstimate(
            flops=12 * width * rows * cols, bytes_accessed=8 * rows * cols, transcendentals=0
        ),
        name="update",
    )(vectors, mixed, dhi, dlo, raw)


def iota(shape, dim):
    return lax.broadcasted_iota(jnp.int32, shape, dim)


def pick_lane(rows, lane):
    hit = iota(rows.shape, 1) == lane
    col = jnp.sum(jnp.where(hit, rows, 0.0), axis=1, keepdims=True)
    return jnp.broadcast_to(col, (rows.shape[0], LANES))


def spread(x, row, width):
    return jnp.broadcast_to(x[row : row + 1, :], (x.shape[0], width))


def widen(x, width):
    return jnp.concatenate([x] * (width // LANES), axis=1)


def cholesky_panel(rows, first):
    count, width = rows.shape
    ri = iota((count, LANES), 0)
    cols = [pick_lane(rows, first + t) for t in range(count)]
    for s in range(count):
        pivot = spread(cols[s], s, LANES)
        root = lax.rsqrt(pivot)
        root = root * (1.5 - 0.5 * pivot * root * root)
        factor = cols[s] * root
        below = jnp.where(ri > s, factor, 0.0)
        row = spread(rows, s, width) * widen(root, width)
        here = iota((count, width), 0) == s
        rows = jnp.where(here, row, rows - widen(below, width) * row)
        for t in range(s + 1, count):
            cols[t] = cols[t] - below * spread(factor, t, LANES)
    return rows


def inverse_panel(rows, first):
    count, width = rows.shape
    ri = iota((count, LANES), 0)
    cols = [pick_lane(rows, first + t) for t in range(count)]
    lane = iota((count, width), 1)
    sub = iota((count, width), 0)
    inside = (lane >= first) & (lane < first + count)
    rows = jnp.where(inside, jnp.where(lane - first == sub, 1.0, 0.0), rows)
    for s in range(count):
        recip = 1.0 / spread(cols[s], s, LANES)
        others = jnp.where(ri == s, 0.0, cols[s])
        row = spread(rows, s, width) * widen(recip, width)
        rows = jnp.where(sub == s, row, rows - widen(others, width) * row)
        for t in range(s + 1, count):
            turn = spread(cols[t], s, LANES) * recip
            cols[t] = jnp.where(ri == s, turn, cols[t] - others * turn)
    return rows


def outer(left, right):
    return lax.dot_general(
        left, right, (((0,), (0,)), ((), ())), precision=lax.Precision.HIGHEST, preferred_element_type=F32
    )


def cholesky_kernel(gram_ref, lower_ref, rest, upper):
    n = gram_ref.shape[1]
    step = 16
    rest[...] = gram_ref[...]

    def body(p, carry):
        first = pl.multiple_of(p * step, step)
        rows = pl.ds(first, step)
        done = [cholesky_panel(rest[k, rows, :], first) for k in range(2)]
        for k in range(2):
            upper[k, rows, :] = done[k]
            rest[k] -= outer(done[k], done[k])
        return carry

    lax.fori_loop(0, n // step, body, 0)
    keep = iota((n, n), 0) >= iota((n, n), 1)
    for k in range(2):
        lower_ref[k] = jnp.where(keep, upper[k].T, 0.0)


def cholesky_pair(gram):
    return pl.pallas_call(
        cholesky_kernel,
        out_shape=jax.ShapeDtypeStruct(gram.shape, F32),
        in_specs=[pl.BlockSpec(memory_space=pltpu.VMEM)],
        out_specs=pl.BlockSpec(memory_space=pltpu.VMEM),
        scratch_shapes=[pltpu.VMEM(gram.shape, F32)] * 2,
        cost_estimate=pl.CostEstimate(flops=10**8, bytes_accessed=10**6, transcendentals=0),
        name="cholesky_pair",
    )(gram)


def inverse_kernel(step, gram_ref, lower_ref, block_ref, out_ref, mat, mat_t):
    n = gram_ref.shape[1]
    left = gram_ref[0] + matmul(lower_ref[0], block_ref[0])
    right = gram_ref[1] + matmul(block_ref[1], lower_ref[1].T)
    mat[0] = left
    mat_t[0] = left.T
    mat[1] = right
    mat_t[1] = right.T

    def body(p, carry):
        first = pl.multiple_of(p * step, step)
        rows = pl.ds(first, step)
        lane = iota((step, n), 1)
        sub = iota((step, n), 0)
        inside = (lane >= first) & (lane < first + step)
        minus = jnp.where(lane - first == sub, -1.0, 0.0)
        wide = [inverse_panel(mat[k, rows, :], first) for k in range(2)]
        tall = [jnp.where(inside, minus, mat_t[k, rows, :]) for k in range(2)]
        ri = iota((n, n), 0)
        ci = iota((n, n), 1)
        clear = ((ri >= first) & (ri < first + step)) | ((ci >= first) & (ci < first + step))
        for k in range(2):
            mat[k] = jnp.where(clear, 0.0, mat[k]) - outer(tall[k], wide[k])
            mat_t[k] = jnp.where(clear, 0.0, mat_t[k]) - outer(wide[k], tall[k])
        return carry

    lax.fori_loop(0, n // step, body, 0)
    out_ref[...] = mat[...]


def inverse_pair(gram, lower, block):
    return pl.pallas_call(
        functools.partial(inverse_kernel, 16),
        out_shape=jax.ShapeDtypeStruct(gram.shape, F32),
        in_specs=[pl.BlockSpec(memory_space=pltpu.VMEM)] * 3,
        out_specs=pl.BlockSpec(memory_space=pltpu.VMEM),
        scratch_shapes=[pltpu.VMEM(gram.shape, F32)] * 2,
        cost_estimate=pl.CostEstimate(flops=10**8, bytes_accessed=10**6, transcendentals=0),
        name="inverse_pair",
    )(gram, lower, block)


MESH = pl.DeviceIdType.MESH
VMEM_SPEC = pl.BlockSpec(memory_space=pltpu.VMEM)
ANY_SPEC = pl.BlockSpec(memory_space=pl.ANY)
DMA = pltpu.SemaphoreType.DMA


def remote(src, dst, send_sem, recv_sem, row, col):
    return pltpu.make_async_remote_copy(
        src_ref=src, dst_ref=dst, send_sem=send_sem, recv_sem=recv_sem, device_id=(row, col), device_id_type=MESH
    )


def bit(x, k):
    return lax.rem(lax.div(x, 2**k), 2)


def log2(n):
    assert n & (n - 1) == 0
    return n.bit_length() - 1


def ring_place(x, n):
    above, place = 0, 0
    for k in reversed(range(log2(n))):
        above = lax.rem(above + bit(x, k), 2)
        place = place + above * 2**k
    return place


def ring_device(place, n):
    x = 0
    for k in range(log2(n)):
        x = x + lax.rem(bit(place, k) + bit(place, k + 1), 2) * 2**k
    return x


def greet(peers, count):
    barrier = pltpu.get_barrier_semaphore()

    def hello(row, col):
        pl.semaphore_signal(barrier, inc=1, device_id=(row, col), device_id_type=MESH)

    for when, row, col in peers:
        if when is None:
            hello(row, col)
        else:
            pl.when(when)(functools.partial(hello, row, col))
    pl.semaphore_wait(barrier, count)


def params(collective_id, vmem=48 * MIB):
    return pltpu.CompilerParams(collective_id=collective_id, has_side_effects=True, vmem_limit_bytes=vmem)


def cross_peers(n_row, n_col, row, col):
    return [(row != r, r, col) for r in range(n_row)] + [(col != c, row, c) for c in range(n_col)]


def broadcast_kernel(n_row, n_col, chunks, panel_in, strip_in, panel_out, strip_out, panel, strip, local, send, recv):
    row, col = lax.axis_index("row"), lax.axis_index("col")
    rows, width = panel.shape[0], strip.shape[0]
    place = ring_place(col, n_col)
    ahead = ring_device(lax.rem(place + 1, n_col), n_col)
    behind = ring_device(lax.rem(place + n_col - 1, n_col), n_col)
    greet(
        [
            (None, row, ahead),
            (None, row, behind),
            (row > 0, row - 1, col),
            (row < n_row - 1, row + 1, col),
        ],
        2 + lax.min(row, 1) + lax.min(n_row - 1 - row, 1),
    )

    @pl.when(place == 0)
    def _():
        load = pltpu.make_async_copy(panel_in, panel, local.at[0])
        load.start()
        load.wait()

    @pl.when(row == n_row - 1)
    def _():
        load = pltpu.make_async_copy(strip_in, strip, local.at[1])
        load.start()
        load.wait()

    half, part, piece = rows // 2, rows // 2 // chunks, width // chunks
    back = lax.rem(n_col - place, n_col)
    streams = (
        (panel, 0, part, place, place > 0, place < n_col - 1, row, ahead),
        (panel, half, part, back, place > 0, place != 1, row, behind),
        (strip, 0, piece, n_row - 1 - row, row < n_row - 1, row > 0, row - 1, col),
    )

    def copy(k, i):
        buf, base, size, _, _, _, to_row, to_col = streams[k]
        where = pl.ds(pl.multiple_of(base + i * size, SUB), size)
        return remote(buf.at[where], buf.at[where], send.at[k, i], recv.at[k, i], to_row, to_col)

    def turn(t, carry):
        for k, (_, _, _, late, gets, gives, _, _) in enumerate(streams):
            i = t - late

            @pl.when((i >= 0) & (i < chunks))
            def _():
                pl.when(gets)(lambda: copy(k, i).wait_recv())
                pl.when(gives)(lambda: copy(k, i).start())

        return carry

    lax.fori_loop(0, chunks + max(n_col, n_row) - 1, turn, 0)
    stores = [
        pltpu.make_async_copy(panel, panel_out, local.at[2]),
        pltpu.make_async_copy(strip, strip_out, local.at[3]),
    ]
    for store in stores:
        store.start()

    def finish(i, carry):
        for k, (_, _, _, _, _, gives, _, _) in enumerate(streams):
            pl.when(gives)(lambda: copy(k, i).wait_send())
        return carry

    lax.fori_loop(0, chunks, finish, 0)
    for store in stores:
        store.wait()


def broadcast_pair(panel, strip, n_row, n_col, collective_id, chunks=8):
    return pl.pallas_call(
        functools.partial(broadcast_kernel, n_row, n_col, chunks),
        out_shape=(
            jax.ShapeDtypeStruct(panel.shape, F32),
            jax.ShapeDtypeStruct(strip.shape, F32),
        ),
        in_specs=[ANY_SPEC] * 2,
        out_specs=(ANY_SPEC, ANY_SPEC),
        scratch_shapes=[
            pltpu.VMEM(panel.shape, F32),
            pltpu.VMEM(strip.shape, F32),
            DMA((4,)),
            DMA((3, chunks)),
            DMA((3, chunks)),
        ],
        compiler_params=params(collective_id),
        cost_estimate=pl.CostEstimate(flops=10**10, bytes_accessed=10**7, transcendentals=0),
        name="broadcast_pair",
    )(panel, strip)


def grams_kernel(
    n_row, n_col, g1, pt, g2, ce, gram_out, block_out,
    part1, part2, left, right, send1, send2, sends, recv1, recv2, recvs, recv_l, recv_r,
):
    row, col = lax.axis_index("row"), lax.axis_index("col")
    width = g1.shape[0]
    qr, qc = width // n_row, width // n_col
    end_row, end_col = n_row - 1, n_col - 1
    greet(cross_peers(n_row, n_col, row, col), n_row + n_col - 2)
    source1, source2 = col == 0, row == end_row

    def first_left(r):
        return remote(g1.at[pl.ds(r * qr, qr)], part1.at[row], send1.at[0, r], recv1.at[row], r, 0)

    def first_top(r):
        return remote(pt.at[pl.ds(r * qr, qr)], left.at[r, 1], send1.at[1, r], recvs.at[0], r, 0)

    def first_right(c):
        return remote(g2.at[pl.ds(c * qc, qc)], part2.at[col], send2.at[0, c], recv2.at[col], end_row, c)

    def first_end(c):
        return remote(ce.at[pl.ds(c * qc, qc)], right.at[c, 1], send2.at[1, c], recvs.at[1], end_row, c)

    def to_col(c):
        return remote(left.at[row], left.at[row], sends.at[0, c], recv_l.at[row], row, c)

    def to_row(r):
        return remote(right.at[col], right.at[col], sends.at[1, r], recv_r.at[col], r, col)

    def spread_left(r):
        return remote(left.at[row], left.at[row], sends.at[2, r], recv_l.at[row], r, col)

    def spread_right(c):
        return remote(right.at[col], right.at[col], sends.at[3, c], recv_r.at[col], row, c)

    def each(count, skip, when, action):
        for k in range(count):
            pl.when(when & (skip != k))(functools.partial(action, k))

    always = row >= 0
    each(n_row, row, source1, lambda r: first_left(r).start())
    each(n_col, col, source2, lambda c: first_right(c).start())
    each(n_row, row, source1 & (row == 0), lambda r: first_top(r).start())
    each(n_col, col, source2 & (col == end_col), lambda c: first_end(c).start())

    @pl.when(source1)
    def _():
        mine = pl.ds(pl.multiple_of(row * qr, SUB), qr)
        part1[row] = g1[mine, :]

        @pl.when(row == 0)
        def _():
            left[0, 1] = pt[0:qr, :]

        for r in range(n_row):
            pl.when(row != r)(
                lambda: remote(part1.at[r], part1.at[r], send1.at[0, r], recv1.at[r], r, 0).wait_recv()
            )
        pl.when(row != 0)(lambda: remote(left.at[row, 1], left.at[row, 1], send1.at[1, 0], recvs.at[0], 0, 0).wait_recv())
        total = part1[0]
        for r in range(1, n_row):
            total = total + part1[r]
        left[row, 0] = total

    each(n_col, 0, source1, lambda c: to_col(c).start())

    @pl.when(source2)
    def _():
        mine = pl.ds(pl.multiple_of(col * qc, SUB), qc)
        part2[col] = g2[mine, :]

        @pl.when(col == end_col)
        def _():
            right[end_col, 1] = ce[end_col * qc : (end_col + 1) * qc, :]

        for c in range(n_col):
            pl.when(col != c)(
                lambda: remote(part2.at[c], part2.at[c], send2.at[0, c], recv2.at[c], end_row, c).wait_recv()
            )
        pl.when(col != end_col)(
            lambda: remote(right.at[col, 1], right.at[col, 1], send2.at[1, 0], recvs.at[1], end_row, 0).wait_recv()
        )
        total = part2[0]
        for c in range(1, n_col):
            total = total + part2[c]
        right[col, 0] = total

    each(n_row, end_row, source2, lambda r: to_row(r).start())

    def got_left(r):
        remote(left.at[r], left.at[r], sends.at[0, 0], recv_l.at[r], row, 0).wait_recv()

    def got_right(c):
        remote(right.at[c], right.at[c], sends.at[1, 0], recv_r.at[c], 0, col).wait_recv()

    pl.when(col != 0)(lambda: got_left(row))
    each(n_row, row, always, lambda r: spread_left(r).start())
    pl.when(row != end_row)(lambda: got_right(col))
    each(n_col, col, always, lambda c: spread_right(c).start())
    each(n_row, row, always, got_left)
    each(n_col, col, always, got_right)
    for r in range(n_row):
        gram_out[0, r * qr : (r + 1) * qr, :] = left[r, 0]
        block_out[0, r * qr : (r + 1) * qr, :] = left[r, 1]
    for c in range(n_col):
        gram_out[1, c * qc : (c + 1) * qc, :] = right[c, 0]
        block_out[1, c * qc : (c + 1) * qc, :] = right[c, 1]
    each(n_row, row, source1, lambda r: first_left(r).wait_send())
    each(n_col, col, source2, lambda c: first_right(c).wait_send())
    each(n_row, row, source1 & (row == 0), lambda r: first_top(r).wait_send())
    each(n_col, col, source2 & (col == end_col), lambda c: first_end(c).wait_send())
    each(n_col, 0, source1, lambda c: to_col(c).wait_send())
    each(n_row, end_row, source2, lambda r: to_row(r).wait_send())
    each(n_row, row, always, lambda r: spread_left(r).wait_send())
    each(n_col, col, always, lambda c: spread_right(c).wait_send())


def share_grams(g1, pt, g2, ce, n_row, n_col, collective_id):
    width = g1.shape[0]
    most = max(n_row, n_col)
    pair = jax.ShapeDtypeStruct((2, width, width), F32)
    return pl.pallas_call(
        functools.partial(grams_kernel, n_row, n_col),
        out_shape=(pair, pair),
        in_specs=[VMEM_SPEC] * 4,
        out_specs=(VMEM_SPEC, VMEM_SPEC),
        scratch_shapes=[
            pltpu.VMEM((n_row, width // n_row, width), F32),
            pltpu.VMEM((n_col, width // n_col, width), F32),
            pltpu.VMEM((n_row, 2, width // n_row, width), F32),
            pltpu.VMEM((n_col, 2, width // n_col, width), F32),
            DMA((2, n_row)),
            DMA((2, n_col)),
            DMA((4, most)),
            DMA((n_row,)),
            DMA((n_col,)),
            DMA((2,)),
            DMA((n_row,)),
            DMA((n_col,)),
        ],
        compiler_params=params(collective_id),
        cost_estimate=pl.CostEstimate(flops=5 * 10**9, bytes_accessed=10**6, transcendentals=0),
        name="share_grams",
    )(g1, pt, g2, ce)


def cross_kernel(n_row, n_col, mine, out, parts, rows, send_r, send_c, recv_r, recv_c):
    row, col = lax.axis_index("row"), lax.axis_index("col")
    count = mine.shape[0]
    greet(cross_peers(n_row, n_col, row, col), n_row + n_col - 2)

    def over_row(r, slot):
        return remote(mine, parts.at[slot], send_r.at[r], recv_r.at[slot], r, col)

    def over_col(c, slot):
        return remote(rows.at[slot], rows.at[slot], send_c.at[c], recv_c.at[slot], row, c)

    for r in range(n_row):
        pl.when(row != r)(lambda: over_row(r, row).start())
    parts[row] = mine[...]
    for r in range(n_row):
        pl.when(row != r)(lambda: over_row(r, r).wait_recv())
    total = parts[0]
    for r in range(1, n_row):
        total = total + parts[r]
    rows[col] = total
    for c in range(n_col):
        pl.when(col != c)(lambda: over_col(c, col).start())
    for c in range(n_col):
        pl.when(col != c)(lambda: over_col(c, c).wait_recv())
    for c in range(n_col):
        out[c * count : (c + 1) * count, :] = rows[c]
    for r in range(n_row):
        pl.when(row != r)(lambda: over_row(r, row).wait_send())
    for c in range(n_col):
        pl.when(col != c)(lambda: over_col(c, col).wait_send())


def sum_cross(part, n_row, n_col, collective_id):
    count, width = part.shape
    return pl.pallas_call(
        functools.partial(cross_kernel, n_row, n_col),
        out_shape=jax.ShapeDtypeStruct((n_col * count, width), F32),
        in_specs=[VMEM_SPEC],
        out_specs=VMEM_SPEC,
        scratch_shapes=[
            pltpu.VMEM((n_row, count, width), F32),
            pltpu.VMEM((n_col, count, width), F32),
            DMA((n_row,)),
            DMA((n_col,)),
            DMA((n_row,)),
            DMA((n_col,)),
        ],
        compiler_params=params(collective_id),
        cost_estimate=pl.CostEstimate(flops=5 * 10**9, bytes_accessed=10**6, transcendentals=0),
        name="sum_cross",
    )(part)


def sum_col_kernel(n_col, part, out, acc, inbox, full, local, send, recv):
    row, col = lax.axis_index("row"), lax.axis_index("col")
    rows = acc.shape[0]
    levels = log2(n_col)
    half = rows // 2
    orders = (list(range(levels)), [0] + list(reversed(range(1, levels))))
    loads = [
        pltpu.make_async_copy(part.at[pl.ds(g * half, half)], acc.at[pl.ds(g * half, half)], local.at[g])
        for g in range(2)
    ]
    for load in loads:
        load.start()
    bits = [bit(col, k) for k in range(levels)]
    partner = [col + (1 - 2 * bits[k]) * 2**k for k in range(levels)]
    greet([(None, row, partner[k]) for k in range(levels)], levels)
    start = [g * half for g in range(2)]
    block = 16
    for load in loads:
        load.wait()

    def reduce_copy(g, j):
        k, size = orders[g][j], half >> (j + 1)
        away = pl.ds(pl.multiple_of(start[g] + (1 - bits[k]) * size, SUB), size)
        slot = pl.ds(half - (half >> j), size)
        return remote(acc.at[away], inbox.at[g, slot], send.at[g, j], recv.at[g, j], row, partner[k])

    sent = []
    for j in range(levels):
        copies = [reduce_copy(g, j) for g in range(2)]
        for copy in copies:
            copy.start()
        sent += copies
        for g in range(2):
            k, size = orders[g][j], half >> (j + 1)
            copies[g].wait_recv()
            kept = start[g] + bits[k] * size
            slot = half - (half >> j)

            goal = full if j == levels - 1 else acc

            def add(i, carry, kept=kept, slot=slot, g=g, goal=goal):
                here = pl.ds(pl.multiple_of(kept + i * block, SUB), block)
                goal[here, :] = acc[here, :] + inbox[g, pl.ds(pl.multiple_of(slot + i * block, SUB), block), :]
                return carry

            lax.fori_loop(0, size // block, add, 0)
            start[g] = kept
    for j in reversed(range(levels)):
        copies = []
        for g in range(2):
            k, size = orders[g][j], half >> (j + 1)
            here = pl.ds(pl.multiple_of(start[g], SUB), size)
            there = pl.ds(pl.multiple_of(start[g] + (1 - 2 * bits[k]) * size, SUB), size)
            slot = levels + j
            out_copy = remote(full.at[here], full.at[here], send.at[g, slot], recv.at[g, slot], row, partner[k])
            in_copy = remote(full.at[there], full.at[there], send.at[g, slot], recv.at[g, slot], row, partner[k])
            copies.append((out_copy, in_copy))
            out_copy.start()
        for g in range(2):
            k, size = orders[g][j], half >> (j + 1)
            copies[g][1].wait_recv()
            start[g] = start[g] - bits[k] * size
            sent.append(copies[g][0])
    store = pltpu.make_async_copy(full, out, local.at[2])
    store.start()
    for copy in sent:
        copy.wait_send()
    store.wait()


def sum_col(part, n_col, collective_id):
    rows, width = part.shape
    levels = log2(n_col)
    half = rows // 2
    return pl.pallas_call(
        functools.partial(sum_col_kernel, n_col),
        out_shape=jax.ShapeDtypeStruct(part.shape, F32),
        in_specs=[ANY_SPEC],
        out_specs=ANY_SPEC,
        scratch_shapes=[
            pltpu.VMEM(part.shape, F32),
            pltpu.VMEM((2, half - half // n_col, width), F32),
            pltpu.VMEM(part.shape, F32),
            DMA((3,)),
            DMA((2, 2 * levels)),
            DMA((2, 2 * levels)),
        ],
        compiler_params=params(collective_id),
        cost_estimate=pl.CostEstimate(flops=2 * 10**10, bytes_accessed=10**7, transcendentals=0),
        name="sum_col",
    )(part)


def on_device(n_row, n_col, pencil_a, pencil_b):
    rows, cols = pencil_a.shape[1], pencil_a.shape[3]
    width = NB
    row, col = lax.axis_index("row"), lax.axis_index("col")
    raw_a = pencil_a.reshape(rows * cols // LANES, LANES)
    raw_b = pencil_b.reshape(rows * cols // LANES, LANES)
    rows_blk = rows // 4
    own_panel = pencil_a[0, :, 0, :width]
    own_strip = pencil_b[0, rows - width :, 0, :]
    gram, block = share_grams(
        matmul(own_panel.T, own_panel),
        own_panel[:width],
        matmul(own_strip, own_strip.T),
        own_strip[:, cols - width :],
        n_row,
        n_col,
        0,
    )
    panel, strip = broadcast_pair(own_panel, own_strip, n_row, n_col, 1)
    lower = cholesky_pair(gram)
    top = jnp.where(row == 0, lower[0].T, 0.0)
    end = jnp.where(col == n_col - 1, lower[1], 0.0)
    vectors = panel + jnp.pad(top, ((0, rows - width), (0, 0)))
    vectors_t = strip + jnp.pad(end, ((0, 0), (cols - width, 0)))
    flipped = vectors.T
    products = [left_products(flipped, raw, rows, cols, rows_blk) for raw in (raw_a, raw_b)]
    products = lax.psum(products, "row")
    inverse = inverse_pair(gram, lower, block)
    mixed = sum_col(right_products(vectors_t.T, raw_a, raw_b, rows, cols, rows_blk), n_col, 2)
    slim = width // n_col
    mine = lax.dynamic_slice(flipped, (col * slim, 0), (slim, rows))
    crossed = sum_cross(jnp.dot(mine, mixed, precision=lax.Precision.HIGH, preferred_element_type=F32), n_row, n_col, 3)
    turned = matmul(inverse[1], vectors_t)
    outs = []
    for side, raw in enumerate((raw_a, raw_b)):
        inner = products[side] - matmul(crossed[:, side * width : (side + 1) * width], turned)
        low = jnp.concatenate([matmul(inverse[0], inner), turned], axis=0)
        outs.append(update(vectors, mixed, side, low, raw, rows, cols, rows_blk))
    return tuple(out.reshape(1, rows, 1, cols) for out in outs)


def solution(mesh):
    placed = (P("row", None, "col", None), P("row", None, "col", None))
    return jax.shard_map(
        functools.partial(on_device, mesh.shape["row"], mesh.shape["col"]),
        mesh=mesh,
        in_specs=placed,
        out_specs=placed,
        check_vma=False,
    )
```
